8 devices in a mesh: dp: 2 (over z, y), pp: 4 (over x, core).
Axes of the slice: x: 2, y: 2, z: 1, core: 2. Of those that a mesh axis runs over, the one named last changes fastest.
Arguments:
- x: bfloat16 [8, 2048, 1024], P(None, 'dp')
- t: bfloat16 [8, 2048, 1024], P(None, 'dp')
- w1: bfloat16 [4, 2, 1024, 4096], P('pp')
- w2: bfloat16 [4, 2, 4096, 1024], P('pp')
Outputs:
- output 1: float32 [4, 2, 1024, 4096], P('pp')
- output 2: float32 [4, 2, 4096, 1024], P('pp')
- output 3: float32 [], replicated
All inputs are finite; a program needn't handle non-finite values.
Results may differ from the reference program's by a relative error of at most 0.00232167.
Values are sent between devices in bfloat16 or wider.
A program may use at most 1 GiB of HBM per device.

```python
import math
import jax
import jax.numpy as jnp
from jax import lax

D = 1024
FF = 4096
STAGES = 4
MICRO = 8
TOKENS = 2048


def _gelu(u):
    c = math.sqrt(2.0 / math.pi)
    return 0.5 * u * (1.0 + jnp.tanh(c * (u + 0.044715 * u * u * u)))


def _dgelu(u):
    c = math.sqrt(2.0 / math.pi)
    th = jnp.tanh(c * (u + 0.044715 * u * u * u))
    return 0.5 * (1.0 + th) + 0.5 * u * (1.0 - th * th) * c * (1.0 + 3.0 * 0.044715 * u * u)


def setup_inputs(seed: int = 0) -> dict:
    k = jax.random.split(jax.random.PRNGKey(seed), 4)
    x = jax.random.normal(k[0], (MICRO, TOKENS, D), jnp.float32)
    t = jax.random.normal(k[1], (MICRO, TOKENS, D), jnp.float32)
    w1 = jax.random.normal(k[2], (STAGES, 2, D, FF), jnp.float32) * D ** -0.5
    w2 = jax.random.normal(k[3], (STAGES, 2, FF, D), jnp.float32) * (FF * STAGES) ** -0.5
    return {'x': x.astype(jnp.bfloat16), 't': t.astype(jnp.bfloat16),
            'w1': w1.astype(jnp.bfloat16), 'w2': w2.astype(jnp.bfloat16)}


def reference(x, t, w1, w2):
    nl = STAGES * 2
    w1f = w1.reshape(nl, D, FF)
    w2f = w2.reshape(nl, FF, D)
    inv = 1.0 / (MICRO * TOKENS * D)

    def fwd(h, w):
        a1, a2 = w
        u = jnp.dot(h, a1, preferred_element_type=jnp.float32).astype(jnp.bfloat16)
        a = _gelu(u.astype(jnp.float32)).astype(jnp.bfloat16)
        h2 = (h.astype(jnp.float32) + jnp.dot(a, a2, preferred_element_type=jnp.float32)).astype(jnp.bfloat16)
        return h2, (h, u)

    def bwd(g, z):
        h, u, a1, a2 = z
        uf = u.astype(jnp.float32)
        a = _gelu(uf).astype(jnp.bfloat16)
        q = jnp.dot(g, a2.T, preferred_element_type=jnp.float32)
        e = (_dgelu(uf) * q).astype(jnp.bfloat16)
        d2 = jnp.dot(a.T, g, preferred_element_type=jnp.float32)
        d1 = jnp.dot(h.T, e, preferred_element_type=jnp.float32)
        g2 = (g.astype(jnp.float32) + jnp.dot(e, a1.T, preferred_element_type=jnp.float32)).astype(jnp.bfloat16)
        return g2, (d1, d2)

    def micro(carry, xt):
        dw1, dw2, loss = carry
        xm, tm = xt
        y, (hs, us) = lax.scan(fwd, xm, (w1f, w2f))
        r = y.astype(jnp.float32) - tm.astype(jnp.float32)
        loss = loss + 0.5 * jnp.sum(r * r) * inv
        g = (r * inv).astype(jnp.bfloat16)
        _, (d1, d2) = lax.scan(bwd, g, (hs, us, w1f, w2f), reverse=True)
        return (dw1 + d1, dw2 + d2, loss), None

    init = (jnp.zeros((nl, D, FF), jnp.float32), jnp.zeros((nl, FF, D), jnp.float32),
            jnp.zeros((), jnp.float32))
    (dw1, dw2, loss), _ = lax.scan(micro, init, (x, t))
    return dw1.reshape(STAGES, 2, D, FF), dw2.reshape(STAGES, 2, FF, D), loss
```

```python
import math
import jax
import jax.numpy as jnp
from jax import lax
from jax.experimental import pallas as pl
from jax.experimental.pallas import tpu as pltpu
from jax.sharding import PartitionSpec as P

MESH = pl.DeviceIdType.MESH
BF = jnp.bfloat16
F32 = jnp.float32
C = math.sqrt(2.0 / math.pi)
K3 = 0.044715
ROWS = 256
LAST_LAG = 6
BURST = 10
PAD = 256
SENDS = 4
PARTS = 4


def _gelu(u):
    z = u * (C + (C * K3) * (u * u))
    return (0.5 * u) * (1.0 + jnp.tanh(z))


def _dgelu_and_gelu(u):
    u2 = u * u
    th = jnp.tanh(u * (C + (C * K3) * u2))
    half = 0.5 * (1.0 + th)
    d = half + (0.5 * u) * (1.0 - th * th) * (C + (3.0 * C * K3) * u2)
    return d, u * half


def _place(q):
    xx = q // 4
    s = (q // 2) % 2
    return ((s + xx) % 2, 2 * xx + q % 2)


def _kernel(inv, x, t, w1, w2,
            hb, ub, ab, eb, gb, tb, ls,
            w1v, w2v, av, hr, lacc, ho, hv, tv, gl, gv, go, uo, ui, ao, eo,
            s_wr, s_ws, s_h, s_g, s_t, s_hl, s_tl, s_gl, s_ul, s_uw, s_aw, s_ew, s_hs, s_gs, s_glw, s_px, s_l, s_lx):
    units, rows, d = hb.shape
    half_units = units // 2
    ff = ub.shape[2]
    dp = lax.axis_index('dp')
    pp = lax.axis_index('pp')
    xx = pp // 2
    c = pp % 2
    s_in = (xx + dp) % 2
    p = 4 * xx + 2 * s_in + c
    first = p == 0
    last = p == 7
    holder = c == s_in
    nxt = _place(jnp.minimum(p + 1, 7))
    prv = _place(jnp.maximum(p - 1, 0))
    lag = LAST_LAG + 6 * (7 - p) + 2 * ((7 - p) // 2)

    barrier = pltpu.get_barrier_semaphore()
    for i in range(1, 8):
        pl.semaphore_signal(barrier, inc=1, device_id=_place((p + i) % 8), device_id_type=MESH)
    pl.semaphore_wait(barrier, 7)

    def cut(ref, n):
        return ref.at[:, pl.ds(0, n)]

    def remote(src, dst, ss, rs, to):
        return pltpu.make_async_remote_copy(src_ref=src, dst_ref=dst, send_sem=ss, recv_sem=rs,
                                            device_id=to, device_id_type=MESH)

    def local(src, dst, sem):
        return pltpu.make_async_copy(src, dst, sem)

    sib = (dp, 2 * xx + 1 - c)

    @pl.when(holder)
    def _():
        local(w1.at[c], cut(w1v, ff), s_wr.at[0]).start()
        local(w2.at[c], cut(w2v, d), s_wr.at[1]).start()
        remote(w1.at[1 - c], cut(w1v, ff), s_ws.at[0], s_wr.at[0], sib).start()
        remote(w2.at[1 - c], cut(w2v, d), s_ws.at[1], s_wr.at[1], sib).start()

    def push(src, dst, base, sem, to, k):
        remote(src.at[k], dst.at[base + k], s_px, sem.at[base + k], to).start()

    def push_all(src, dst, base, sem, to, n):
        def step(k, carry):
            push(src, dst, base, sem, to, k)
            return carry
        lax.fori_loop(0, n, step, 0)

    @pl.when(p == 1)
    def _():
        push_all(x, hb, 0, s_h, _place(0), half_units)

    @pl.when(p == 3)
    def _():
        push_all(x, hb, half_units, s_h, _place(0), half_units)

    @pl.when(p == 6)
    def _():
        push_all(t, tb, 0, s_t, _place(7), half_units)

    @pl.when(p == 4)
    def _():
        push_all(t, tb, half_units, s_t, _place(7), BURST)

    def paced_push(k):
        j = BURST - 1 + k // 2

        @pl.when((p == 4) & (k >= 2) & (k % 2 == 0) & (j < half_units))
        def _():
            push(t, tb, half_units, s_t, _place(7), j)

    lacc[...] = jnp.zeros_like(lacc)
    local(w1.at[c], cut(w1v, ff), s_wr.at[0]).wait()
    local(w2.at[c], cut(w2v, d), s_wr.at[1]).wait()

    nt = (((1,), (1,)), ((), ()))
    nc, no = ff // PARTS, d // PARTS

    def f1(s, j):
        sl, so = slice(j * nc, (j + 1) * nc), slice(j * no, (j + 1) * no)
        u = jnp.dot(hv[s, :, :d], w1v[:, sl], preferred_element_type=F32).astype(BF)
        uo[s, :, sl] = u
        av[:, sl] = _gelu(u.astype(F32)).astype(BF)
        hr[:, so] = hv[s, :, so]

    def f2(k, s, j):
        sl = slice(j * no, (j + 1) * no)
        acc = jnp.dot(av[:, :ff], w2v[:, sl], preferred_element_type=F32)
        y = (hr[:, sl].astype(F32) + acc).astype(BF)
        ho[k % SENDS, :, sl] = y
        r = y.astype(F32) - tv[s, :, sl].astype(F32)
        gl[s, :, sl] = (r * inv).astype(BF)
        lacc[:, sl] += jnp.sum((r * r).reshape(rows // 8, 8, no), axis=0)

    def b1(s, j):
        sl = slice(j * nc, (j + 1) * nc)
        q = lax.dot_general(gv[s, :, :d], w2v[sl, :d], nt, preferred_element_type=F32)
        dg, a = _dgelu_and_gelu(ui[s, :, sl].astype(F32))
        ao[s, :, sl] = a.astype(BF)
        eo[s, :, sl] = (dg * q).astype(BF)

    def b2(s, j):
        sl = slice(j * no, (j + 1) * no)
        acc = lax.dot_general(eo[s, :, :ff], w1v[sl, :ff], nt, preferred_element_type=F32)
        go[s, :, sl] = (gv[s, :, sl].astype(F32) + acc).astype(BF)

    def h_load(k, s):
        return local(hb.at[k], cut(hv.at[s], d), s_hl.at[s])

    def t_load(k, s):
        return local(tb.at[k], cut(tv.at[s], d), s_tl.at[s])

    def g_load(m, s):
        return local(gb.at[m], cut(gv.at[s], d), s_gl.at[s])

    def u_load(m, s):
        return local(ub.at[m], cut(ui.at[s], ff), s_ul.at[s])

    def u_write(k, s):
        return local(cut(uo.at[s], ff), ub.at[k], s_uw.at[s])

    def a_write(m, s):
        return local(cut(ao.at[s], ff), ab.at[m], s_aw.at[s])

    def e_write(m, s):
        return local(cut(eo.at[s], ff), eb.at[m], s_ew.at[s])

    def gl_write(k, s):
        return local(cut(gl.at[s], d), gb.at[k], s_glw.at[s])

    def h_send(k, s):
        return remote(ho.at[k % SENDS, :, pl.ds(0, d)], hb.at[k], s_hs.at[k % SENDS], s_h.at[k], nxt)

    def g_send(m, s):
        return remote(cut(go.at[s], d), gb.at[m], s_gs.at[s], s_g.at[m], prv)

    def fetch_h(k, s):
        local(hb.at[k], hb.at[k], s_h.at[k]).wait()
        h_load(k, s).start()

    def fetch_t(k, s):
        @pl.when(last)
        def _():
            local(tb.at[k], tb.at[k], s_t.at[k]).wait()
            t_load(k, s).start()

    def fetch_g(m, s):
        @pl.when(jnp.logical_not(last))
        def _():
            local(gb.at[m], gb.at[m], s_g.at[m]).wait()
        g_load(m, s).start()

    def wait_t(k, s):
        @pl.when(last)
        def _():
            t_load(k, s).wait()

    def wait_gl(k, s):
        @pl.when(last & (k >= 0))
        def _():
            gl_write(k, s).wait()

    def wait_h_send(k, s):
        @pl.when(jnp.logical_not(last) & (k >= 0))
        def _():
            h_send(k, s).wait_send()

    def wait_b_outputs(m, s):
        a_write(m, s).wait()
        e_write(m, s).wait()

        @pl.when(p > 0)
        def _():
            g_send(m, s).wait_send()

    def put_f(k, s):
        @pl.when(last)
        def _():
            gl_write(k, s).start()

        @pl.when(jnp.logical_not(last))
        def _():
            h_send(k, s).start()

    def put_b(m, s):
        @pl.when(p > 0)
        def _():
            g_send(m, s).start()

    def warm(k, carry):
        s = k % 2
        paced_push(k)
        h_load(k, s).wait()
        wait_t(k, s)

        @pl.when(k >= 2)
        def _():
            u_write(k - 2, s).wait()
        wait_gl(k - 2, s)
        wait_h_send(k - SENDS, s)
        for j in range(PARTS):
            f1(s, j)
        for j in range(PARTS):
            f2(k, s, j)
        put_f(k, s)
        u_write(k, s).start()
        fetch_h(k + 1, 1 - s)
        fetch_t(k + 1, 1 - s)
        return carry

    def steady(i, carry):
        for s in (0, 1):
            m = 2 * i + s
            k = lag + m
            paced_push(k)
            h_load(k, s).wait()
            wait_t(k - 1, 1 - s)
            g_load(m, s).wait()
            u_load(m, s).wait()
            u_write(k - 2, s).wait()
            wait_gl(k - 3, 1 - s)
            wait_h_send(k - 1 - SENDS, 1 - s)

            @pl.when(m >= 2)
            def _():
                wait_b_outputs(m - 2, s)
            u_load(m + 1, 1 - s).start()

            @pl.when(k + 1 < units)
            def _():
                fetch_h(k + 1, 1 - s)
            fetch_t(k, s)
            fetch_g(m + 1, 1 - s)
            for j in range(PARTS):
                f2(k - 1, 1 - s, j)
                b1(s, j)
            for j in range(PARTS):
                b2(s, j)
                f1(s, j)
            put_f(k - 1, 1 - s)
            put_b(m, s)
            u_write(k, s).start()
            e_write(m, s).start()
            a_write(m, s).start()
        return carry

    def cool(i, carry):
        m = units - lag + i
        s = m % 2
        g_load(m, s).wait()
        u_load(m, s).wait()

        @pl.when(m >= 2)
        def _():
            wait_b_outputs(m - 2, s)

        @pl.when(m + 1 < units)
        def _():
            u_load(m + 1, 1 - s).start()
        for j in range(PARTS):
            b1(s, j)
        for j in range(PARTS):
            b2(s, j)
        put_b(m, s)
        e_write(m, s).start()
        a_write(m, s).start()

        @pl.when(m + 1 < units)
        def _():
            fetch_g(m + 1, 1 - s)
        return carry

    fetch_h(0, 0)
    fetch_t(0, 0)
    lax.fori_loop(0, lag - 1, warm, 0)

    h_load(lag - 1, 1).wait()
    u_write(lag - 3, 1).wait()
    for j in range(PARTS):
        f1(1, j)
    u_write(lag - 1, 1).start()
    fetch_h(lag, 0)
    u_load(0, 0).start()
    fetch_g(0, 0)
    lax.fori_loop(0, (units - lag) // 2, steady, 0)

    wait_t(units - 1, 1)
    wait_gl(units - 3, 1)
    wait_h_send(units - 1 - SENDS, 1)
    for j in range(PARTS):
        f2(units - 1, 1, j)
    put_f(units - 1, 1)
    u_write(units - 2, 0).wait()
    u_write(units - 1, 1).wait()
    wait_gl(units - 2, 0)
    wait_gl(units - 1, 1)

    @pl.when(last)
    def _():
        local(lacc, ls, s_l).start()
        for i in range(7):
            remote(lacc, ls, s_lx.at[i], s_l, _place(i)).start()

    lax.fori_loop(0, lag, cool, 0)
    for i in range(SENDS):
        wait_h_send(units - SENDS + i, i % 2)
    wait_b_outputs(units - 2, 0)
    wait_b_outputs(units - 1, 1)
    local(lacc, ls, s_l).wait()

    @pl.when(last)
    def _():
        for i in range(7):
            remote(lacc, ls, s_lx.at[i], s_l, _place(i)).wait_send()

    @pl.when(holder)
    def _():
        remote(w1.at[1 - c], cut(w1v, ff), s_ws.at[0], s_wr.at[0], sib).wait_send()
        remote(w2.at[1 - c], cut(w2v, d), s_ws.at[1], s_wr.at[1], sib).wait_send()

    @pl.when((p == 1) | (p == 3))
    def _():
        remote(x, hb.at[pl.ds(0, half_units)], s_px, s_h.at[0], _place(0)).wait_send()

    @pl.when((p == 4) | (p == 6))
    def _():
        remote(t, tb.at[pl.ds(0, half_units)], s_px, s_t.at[0], _place(7)).wait_send()


def _forward_backward(x, t, w1, w2, inv):
    half_units, rows, d = x.shape
    units = 2 * half_units
    ff = w1.shape[-1]
    any_ = pl.BlockSpec(memory_space=pl.ANY)
    dw, fw = d + PAD, ff + PAD
    small = [pltpu.VMEM((2, rows, dw), BF)]
    big = [pltpu.VMEM((2, rows, fw), BF)]
    dma = pltpu.SemaphoreType.DMA
    narrow = jax.ShapeDtypeStruct((units, rows, d), BF)
    wide = jax.ShapeDtypeStruct((units, rows, ff), BF)

    def kern(*refs):
        _kernel(inv, *refs)

    flops = 8 * units * rows * d * ff
    return pl.pallas_call(
        kern,
        out_shape=(narrow, wide, wide, wide, narrow, narrow, jax.ShapeDtypeStruct((8, d), F32)),
        in_specs=[any_] * 4,
        out_specs=[any_] * 7,
        scratch_shapes=[
            pltpu.VMEM((d, fw), BF), pltpu.VMEM((ff, dw), BF), pltpu.VMEM((rows, fw), BF),
            pltpu.VMEM((rows, dw), BF), pltpu.VMEM((8, d), F32), pltpu.VMEM((SENDS, rows, dw), BF),
            *(small * 5), *(big * 4),
            dma((2,)), dma((2,)), dma((units,)), dma((units,)), dma((units,)),
            dma((2,)), dma((2,)), dma((2,)), dma((2,)), dma((2,)), dma((2,)), dma((2,)),
            dma((SENDS,)), dma((2,)), dma((2,)), dma(()), dma(()), dma((7,)),
        ],
        compiler_params=pltpu.CompilerParams(collective_id=0, has_side_effects=True, vmem_limit_bytes=67043328),
        cost_estimate=pl.CostEstimate(flops=flops, bytes_accessed=10 * units * rows * ff, transcendentals=0),
    )(x, t, w1, w2)


def solution(mesh):
    def flat(x, y, c):
        return y * 4 + 2 * x + c

    keep = [[(flat(x, y, j), flat(x, y, 1 - j)) for x in (0, 1) for y in (0, 1) if (x + y) % 2 != j] for j in (0, 1)]
    swap = [[(flat(x, y, j), flat(x, 1 - y, (x + y) % 2)) for x in (0, 1) for y in (0, 1)] for j in (0, 1)]

    def body(x, t, w1, w2):
        nm, tok, d = x.shape
        ff = w1.shape[-1]
        ndp = 2
        inv = 1.0 / (nm * tok * ndp * d)
        pp = lax.axis_index('pp')
        own = (pp // 2 + lax.axis_index('dp')) % 2 == pp % 2
        xs = x.reshape(nm * tok // ROWS, ROWS, d)
        ts = t.reshape(nm * tok // ROWS, ROWS, d)
        hb, _, ab, eb, gb, _, ls = _forward_backward(xs, ts, w1[0], w2[0], inv)
        n = hb.shape[0] * ROWS
        h, g = hb.reshape(n, d), gb.reshape(n, d)
        a, e = ab.reshape(n, ff), eb.reshape(n, ff)

        dw1 = jnp.zeros((2, d, ff), F32)
        dw2 = jnp.zeros((2, ff, d), F32)

        def spread(v):
            out = []
            for j in (0, 1):
                here = lax.ppermute(v, ('dp', 'pp'), keep[j])
                there = lax.ppermute(v, ('dp', 'pp'), swap[j])
                out.append(jnp.where(own, jnp.where(pp % 2 == j, v, here), there))
            return out

        c0 = 0
        for cs in (256, 512, 768, 1024, 1024, 512):
            v = lax.dot_general(h, e[:, c0:c0 + cs], (((0,), (0,)), ((), ())), preferred_element_type=F32)
            for j, part in enumerate(spread(v)):
                dw1 = lax.dynamic_update_slice(dw1, part[None], (j, 0, c0))
            c0 += cs
        c0 = 0
        for cs in (1024, 1024, 1024, 512, 512):
            v = lax.dot_general(a[:, c0:c0 + cs], g, (((0,), (0,)), ((), ())), preferred_element_type=F32)
            for j, part in enumerate(spread(v)):
                dw2 = lax.dynamic_update_slice(dw2, part[None], (j, c0, 0))
            c0 += cs
        loss = 0.5 * inv * jnp.sum(ls)
        return dw1[None], dw2[None], loss

    return jax.shard_map(body, mesh=mesh,
                         in_specs=(P(None, 'dp', None), P(None, 'dp', None), P('pp'), P('pp')),
                         out_specs=(P('pp'), P('pp'), P()), check_vma=False)
```

```python
import functools
import math
import jax
import jax.numpy as jnp
from jax import lax
from jax.experimental import pallas as pl
from jax.experimental.pallas import tpu as pltpu
from jax.sharding import PartitionSpec as P

MESH = pl.DeviceIdType.MESH
BF = jnp.bfloat16
F32 = jnp.float32
C = math.sqrt(2.0 / math.pi)
K3 = 0.044715
ROWS = 256
LAST_LAG = 4
BURST = 13
PAD = 256
SENDS = 4
PARTS = 4
KBLOCK = 1024
TILE1 = 512
TILE2 = 256
SLOTS = 4
DEPTH = 4


def _gelu(u):
    z = u * (C + (C * K3) * (u * u))
    return (0.5 * u) * (1.0 + jnp.tanh(z))


def _dgelu_and_gelu(u):
    u2 = u * u
    th = jnp.tanh(u * (C + (C * K3) * u2))
    half = 0.5 * (1.0 + th)
    d = half + (0.5 * u) * (1.0 - th * th) * (C + (3.0 * C * K3) * u2)
    return d, u * half


def _place(q):
    xx = q // 4
    s = (q // 2) % 2
    return ((s + xx) % 2, 2 * xx + q % 2)


def _kernel(inv, x, t, w1, w2,
            hb, ub, ab, eb, gb, tb, wb1, wb2, ls,
            w1v, w2v, av, hr, lacc, ho, hv, tv, gl, gv, go, uo, ui, ao, eo,
            s_wr, s_ws, s_h, s_g, s_t, s_hl, s_tl, s_gl, s_ul, s_uw, s_aw, s_ew, s_hs, s_gs, s_glw, s_px, s_l, s_lx, s_wl):
    units, rows, d = hb.shape
    half_units = units // 2
    ff = ub.shape[2]
    dp = lax.axis_index('dp')
    pp = lax.axis_index('pp')
    xx = pp // 2
    c = pp % 2
    s_in = (xx + dp) % 2
    p = 4 * xx + 2 * s_in + c
    first = p == 0
    last = p == 7
    holder = c == s_in
    nxt = _place(jnp.minimum(p + 1, 7))
    prv = _place(jnp.maximum(p - 1, 0))
    lag = LAST_LAG + 6 * (7 - p) + 2 * ((7 - p) // 2)

    barrier = pltpu.get_barrier_semaphore()
    for i in range(1, 8):
        pl.semaphore_signal(barrier, inc=1, device_id=_place((p + i) % 8), device_id_type=MESH)
    pl.semaphore_wait(barrier, 7)

    def cut(ref, n):
        return ref.at[:, pl.ds(0, n)]

    def remote(src, dst, ss, rs, to):
        return pltpu.make_async_remote_copy(src_ref=src, dst_ref=dst, send_sem=ss, recv_sem=rs,
                                            device_id=to, device_id_type=MESH)

    def local(src, dst, sem):
        return pltpu.make_async_copy(src, dst, sem)

    sib = (dp, 2 * xx + 1 - c)

    @pl.when(holder)
    def _():
        local(w1.at[c], cut(w1v, ff), s_wr.at[0]).start()
        local(w2.at[c], cut(w2v, d), s_wr.at[1]).start()
        remote(w1.at[1 - c], wb1, s_ws.at[0], s_wr.at[0], sib).start()
        remote(w2.at[1 - c], wb2, s_ws.at[1], s_wr.at[1], sib).start()

    def push(src, dst, base, sem, to, k):
        remote(src.at[k], dst.at[base + k], s_px, sem.at[base + k], to).start()

    def push_all(src, dst, base, sem, to, n):
        def step(k, carry):
            push(src, dst, base, sem, to, k)
            return carry
        lax.fori_loop(0, n, step, 0)

    @pl.when(p == 1)
    def _():
        push_all(x, hb, 0, s_h, _place(0), half_units)

    @pl.when(p == 3)
    def _():
        push_all(x, hb, half_units, s_h, _place(0), half_units)

    @pl.when(p == 6)
    def _():
        push_all(t, tb, 0, s_t, _place(7), half_units)

    @pl.when(p == 4)
    def _():
        push_all(t, tb, half_units, s_t, _place(7), BURST)

    def paced_push(m):
        j = BURST + m // 2

        @pl.when((p == 4) & (j < half_units))
        def _():
            push(t, tb, half_units, s_t, _place(7), j)

    lacc[...] = jnp.zeros_like(lacc)
    local(w1.at[c], cut(w1v, ff), s_wr.at[0]).wait()

    @pl.when(jnp.logical_not(holder))
    def _():
        local(wb1, cut(w1v, ff), s_wl.at[0]).start()
    local(w2.at[c], cut(w2v, d), s_wr.at[1]).wait()

    @pl.when(jnp.logical_not(holder))
    def _():
        local(wb2, cut(w2v, d), s_wl.at[1]).start()
        local(wb1, cut(w1v, ff), s_wl.at[0]).wait()
        local(wb2, cut(w2v, d), s_wl.at[1]).wait()

    nt = (((1,), (1,)), ((), ()))
    nc, no = ff // PARTS, d // PARTS

    def f1(s, j):
        sl, so = slice(j * nc, (j + 1) * nc), slice(j * no, (j + 1) * no)
        u = jnp.dot(hv[s, :, :d], w1v[:, sl], preferred_element_type=F32).astype(BF)
        uo[s, :, sl] = u
        av[:, sl] = _gelu(u.astype(F32)).astype(BF)
        hr[:, so] = hv[s, :, so]

    def f2(k, s, j):
        sl = slice(j * no, (j + 1) * no)
        acc = jnp.dot(av[:, :ff], w2v[:, sl], preferred_element_type=F32)
        y = (hr[:, sl].astype(F32) + acc).astype(BF)
        ho[k % SENDS, :, sl] = y
        r = y.astype(F32) - tv[s, :, sl].astype(F32)
        gl[s, :, sl] = (r * inv).astype(BF)
        lacc[:, sl] += jnp.sum((r * r).reshape(rows // 8, 8, no), axis=0)

    def b1(s, j):
        sl = slice(j * nc, (j + 1) * nc)
        q = lax.dot_general(gv[s, :, :d], w2v[sl, :d], nt, preferred_element_type=F32)
        dg, a = _dgelu_and_gelu(ui[s, :, sl].astype(F32))
        ao[s, :, sl] = a.astype(BF)
        eo[s, :, sl] = (dg * q).astype(BF)

    def b2(s, j):
        sl = slice(j * no, (j + 1) * no)
        acc = lax.dot_general(eo[s, :, :ff], w1v[sl, :ff], nt, preferred_element_type=F32)
        go[s, :, sl] = (gv[s, :, sl].astype(F32) + acc).astype(BF)

    def h_load(k, s):
        return local(hb.at[k], cut(hv.at[s], d), s_hl.at[s])

    def t_load(k, s):
        return local(tb.at[k], cut(tv.at[s], d), s_tl.at[s])

    def g_load(m, s):
        return local(gb.at[m], cut(gv.at[s], d), s_gl.at[s])

    def u_load(m, s):
        return local(ub.at[m], cut(ui.at[s], ff), s_ul.at[s])

    def u_write(k, s):
        return local(cut(uo.at[s], ff), ub.at[k], s_uw.at[s])

    def a_write(m, s):
        return local(cut(ao.at[s], ff), ab.at[m], s_aw.at[s])

    def e_write(m, s):
        return local(cut(eo.at[s], ff), eb.at[m], s_ew.at[s])

    def gl_write(k, s):
        return local(cut(gl.at[s], d), gb.at[k], s_glw.at[s])

    def h_send(k, s):
        return remote(ho.at[k % SENDS, :, pl.ds(0, d)], hb.at[k], s_hs.at[k % SENDS], s_h.at[k], nxt)

    def g_send(m, s):
        return remote(cut(go.at[s], d), gb.at[m], s_gs.at[s], s_g.at[m], prv)

    def fetch_h(k, s):
        local(hb.at[k], hb.at[k], s_h.at[k]).wait()
        h_load(k, s).start()

    def fetch_t(k, s):
        @pl.when(last)
        def _():
            local(tb.at[k], tb.at[k], s_t.at[k]).wait()
            t_load(k, s).start()

    def fetch_g(m, s):
        @pl.when(jnp.logical_not(last))
        def _():
            local(gb.at[m], gb.at[m], s_g.at[m]).wait()
        g_load(m, s).start()

    def wait_t(k, s):
        @pl.when(last)
        def _():
            t_load(k, s).wait()

    def wait_gl(k, s):
        @pl.when(last & (k >= 0))
        def _():
            gl_write(k, s).wait()

    def wait_h_send(k, s):
        @pl.when(jnp.logical_not(last) & (k >= 0))
        def _():
            h_send(k, s).wait_send()

    def wait_b_outputs(m, s):
        a_write(m, s).wait()
        e_write(m, s).wait()

        @pl.when(p > 0)
        def _():
            g_send(m, s).wait_send()

    def put_f(k, s):
        @pl.when(last)
        def _():
            gl_write(k, s).start()

        @pl.when(jnp.logical_not(last))
        def _():
            h_send(k, s).start()

    def put_b(m, s):
        @pl.when(p > 0)
        def _():
            g_send(m, s).start()

    def warm(k, carry):
        s = k % 2
        h_load(k, s).wait()
        wait_t(k, s)

        @pl.when(k >= 2)
        def _():
            u_write(k - 2, s).wait()
        wait_gl(k - 2, s)
        wait_h_send(k - SENDS, s)
        for j in range(PARTS):
            f1(s, j)
        for j in range(PARTS):
            f2(k, s, j)
        put_f(k, s)
        u_write(k, s).start()
        fetch_h(k + 1, 1 - s)
        fetch_t(k + 1, 1 - s)
        return carry

    def steady(i, carry):
        for s in (0, 1):
            m = 2 * i + s
            k = lag + m
            if s == 0:
                paced_push(m)
            h_load(k, s).wait()
            wait_t(k - 1, 1 - s)
            g_load(m, s).wait()
            u_load(m, s).wait()
            u_write(k - 2, s).wait()
            wait_gl(k - 3, 1 - s)
            wait_h_send(k - 1 - SENDS, 1 - s)

            @pl.when(m >= 2)
            def _():
                wait_b_outputs(m - 2, s)
            u_load(m + 1, 1 - s).start()

            @pl.when(k + 1 < units)
            def _():
                fetch_h(k + 1, 1 - s)
            fetch_t(k, s)
            fetch_g(m + 1, 1 - s)
            for j in range(PARTS):
                f2(k - 1, 1 - s, j)
                b1(s, j)
            for j in range(PARTS):
                b2(s, j)
                f1(s, j)
            put_f(k - 1, 1 - s)
            put_b(m, s)
            u_write(k, s).start()
            e_write(m, s).start()
            a_write(m, s).start()
        return carry

    def cool(i, carry):
        m = units - lag + i
        s = m % 2
        g_load(m, s).wait()
        u_load(m, s).wait()

        @pl.when(m >= 2)
        def _():
            wait_b_outputs(m - 2, s)

        @pl.when(m + 1 < units)
        def _():
            u_load(m + 1, 1 - s).start()
        for j in range(PARTS):
            b1(s, j)
        for j in range(PARTS):
            b2(s, j)
        put_b(m, s)
        e_write(m, s).start()
        a_write(m, s).start()

        @pl.when(m + 1 < units)
        def _():
            fetch_g(m + 1, 1 - s)
        return carry

    fetch_h(0, 0)
    fetch_t(0, 0)
    lax.fori_loop(0, lag - 1, warm, 0)

    h_load(lag - 1, 1).wait()
    u_write(lag - 3, 1).wait()
    for j in range(PARTS):
        f1(1, j)
    u_write(lag - 1, 1).start()
    fetch_h(lag, 0)
    u_load(0, 0).start()
    fetch_g(0, 0)
    lax.fori_loop(0, (units - lag) // 2, steady, 0)

    wait_t(units - 1, 1)
    wait_gl(units - 3, 1)
    wait_h_send(units - 1 - SENDS, 1)
    for j in range(PARTS):
        f2(units - 1, 1, j)
    put_f(units - 1, 1)
    u_write(units - 2, 0).wait()
    u_write(units - 1, 1).wait()
    wait_gl(units - 2, 0)
    wait_gl(units - 1, 1)

    @pl.when(last)
    def _():
        local(lacc, ls, s_l).start()
        for i in range(7):
            remote(lacc, ls, s_lx.at[i], s_l, _place(i)).start()

    lax.fori_loop(0, lag, cool, 0)
    for i in range(SENDS):
        wait_h_send(units - SENDS + i, i % 2)
    wait_b_outputs(units - 2, 0)
    wait_b_outputs(units - 1, 1)
    local(lacc, ls, s_l).wait()

    @pl.when(last)
    def _():
        for i in range(7):
            remote(lacc, ls, s_lx.at[i], s_l, _place(i)).wait_send()

    @pl.when(holder)
    def _():
        remote(w1.at[1 - c], wb1, s_ws.at[0], s_wr.at[0], sib).wait_send()
        remote(w2.at[1 - c], wb2, s_ws.at[1], s_wr.at[1], sib).wait_send()

    @pl.when((p == 1) | (p == 3))
    def _():
        remote(x, hb.at[pl.ds(0, half_units)], s_px, s_h.at[0], _place(0)).wait_send()

    @pl.when((p == 4) | (p == 6))
    def _():
        remote(t, tb.at[pl.ds(0, half_units)], s_px, s_t.at[0], _place(7)).wait_send()


def _forward_backward(x, t, w1, w2, inv):
    half_units, rows, d = x.shape
    units = 2 * half_units
    ff = w1.shape[-1]
    any_ = pl.BlockSpec(memory_space=pl.ANY)
    dw, fw = d + PAD, ff + PAD
    small = [pltpu.VMEM((2, rows, dw), BF)]
    big = [pltpu.VMEM((2, rows, fw), BF)]
    dma = pltpu.SemaphoreType.DMA
    narrow = jax.ShapeDtypeStruct((units, rows, d), BF)
    wide = jax.ShapeDtypeStruct((units, rows, ff), BF)

    def kern(*refs):
        _kernel(inv, *refs)

    flops = 8 * units * rows * d * ff
    return pl.pallas_call(
        kern,
        out_shape=(narrow, wide, wide, wide, narrow, narrow, jax.ShapeDtypeStruct((d, ff), BF),
                   jax.ShapeDtypeStruct((ff, d), BF), jax.ShapeDtypeStruct((8, d), F32)),
        in_specs=[any_] * 4,
        out_specs=[any_] * 9,
        scratch_shapes=[
            pltpu.VMEM((d, fw), BF), pltpu.VMEM((ff, dw), BF), pltpu.VMEM((rows, fw), BF),
            pltpu.VMEM((rows, dw), BF), pltpu.VMEM((8, d), F32), pltpu.VMEM((SENDS, rows, dw), BF),
            *(small * 5), *(big * 4),
            dma((2,)), dma((2,)), dma((units,)), dma((units,)), dma((units,)),
            dma((2,)), dma((2,)), dma((2,)), dma((2,)), dma((2,)), dma((2,)), dma((2,)),
            dma((SENDS,)), dma((2,)), dma((2,)), dma(()), dma(()), dma((7,)), dma((2,)),
        ],
        compiler_params=pltpu.CompilerParams(collective_id=0, has_side_effects=True, vmem_limit_bytes=67043328),
        cost_estimate=pl.CostEstimate(flops=flops, bytes_accessed=10 * units * rows * ff, transcendentals=0),
    )(x, t, w1, w2)


def _grad_kernel(h, e, a, g, dw1, dw2, rest, narrow, wide1, wide2, acc1, acc2, s_n, s_w, s_keep, s_send, s_in):
    tokens, d = h.shape
    ff = e.shape[1]
    blocks = tokens // KBLOCK
    dp = lax.axis_index('dp')
    pp = lax.axis_index('pp')
    xx = pp // 2
    c = pp % 2
    side = (xx + dp) % 2
    own = c == side
    here = (dp, 2 * xx + side)
    there = (1 - dp, 2 * xx + side)

    barrier = pltpu.get_barrier_semaphore()
    for i in range(1, 4):
        to = ((dp + i // 2) % 2, 2 * xx + (c + i) % 2)
        pl.semaphore_signal(barrier, inc=1, device_id=to, device_id_type=MESH)
    pl.semaphore_wait(barrier, 3)

    def phase(thin, fat, wide, acc, out, cols, arr):
        tile = wide.shape[-1]
        tiles = ff // tile
        sent = tiles - 1 if cols else tiles

        def load(t, s):
            k = pl.multiple_of((t % blocks) * KBLOCK, KBLOCK)
            n = pl.multiple_of((t // blocks) * tile, tile)
            return (pltpu.make_async_copy(thin.at[pl.ds(k, KBLOCK)], narrow.at[s], s_n.at[s]),
                    pltpu.make_async_copy(fat.at[pl.ds(k, KBLOCK), pl.ds(n, tile)], wide.at[s], s_w.at[s]))

        def place(i):
            n = pl.multiple_of(i * tile, tile)
            return out.at[c, :, pl.ds(n, tile)] if cols else out.at[c, pl.ds(n, tile)]

        def keep_local(i, slot):
            return pltpu.make_async_copy(acc.at[slot], place(i), s_keep.at[arr, slot])

        def keep_remote(i, slot):
            return pltpu.make_async_remote_copy(acc.at[slot], place(i), s_keep.at[arr, slot], s_in.at[arr, c],
                                                device_id=here, device_id_type=MESH)

        def send(i, slot):
            return pltpu.make_async_remote_copy(acc.at[slot], place(i), s_send.at[arr, slot], s_in.at[arr, c],
                                                device_id=there, device_id_type=MESH)

        def rest_local(slot):
            return pltpu.make_async_copy(acc.at[slot], rest, s_keep.at[arr, slot])

        def drain(i, slot):
            send(i, slot).wait_send()

            @pl.when(jnp.logical_not(own))
            def _():
                keep_remote(i, slot).wait_send()

            @pl.when(own)
            def _():
                keep_local(i, slot).wait()

        for ahead in range(DEPTH - 1):
            for cp in load(ahead, ahead):
                cp.start()

        def step(t, carry):
            s = t % DEPTH
            i = t // blocks
            k = t % blocks
            slot = i % SLOTS

            @pl.when(k == 0)
            def _():
                @pl.when(i >= SLOTS)
                def _():
                    drain(i - SLOTS, slot)
                acc[slot] = jnp.zeros(acc.shape[1:], F32)
            for cp in load(t, s):
                cp.wait()

            @pl.when(t + DEPTH - 1 < tiles * blocks)
            def _():
                for cp in load(t + DEPTH - 1, (t + DEPTH - 1) % DEPTH):
                    cp.start()
            lhs, rhs = (narrow, wide) if cols else (wide, narrow)
            for q in range(acc.shape[1] // 256):
                rows = slice(q * 256, (q + 1) * 256)
                acc[slot, rows, :] += lax.dot_general(lhs[s, :, rows], rhs[s], (((0,), (0,)), ((), ())),
                                                      preferred_element_type=F32)

            if sent < tiles:
                @pl.when(t == tiles * blocks - 1)
                def _():
                    rest_local(slot).start()

            @pl.when((k == blocks - 1) & (i < sent))
            def _():
                send(i, slot).start()

                @pl.when(own)
                def _():
                    keep_local(i, slot).start()

                @pl.when(jnp.logical_not(own))
                def _():
                    keep_remote(i, slot).start()
            return carry

        lax.fori_loop(0, tiles * blocks, step, 0)
        for i in range(tiles - SLOTS, sent):
            late.append(functools.partial(drain, i, i % SLOTS))
        if sent < tiles:
            late.append(lambda: rest_local((tiles - 1) % SLOTS).wait())

    late = []
    phase(g, a, wide2, acc2, dw2, False, 1)
    phase(h, e, wide1, acc1, dw1, True, 0)
    for wait in late:
        wait()

    for j in (0, 1):
        @pl.when(jnp.logical_not(own) | (c != j))
        def _():
            part = dw1.at[j, :, pl.ds(0, ff - TILE1)]
            pltpu.make_async_copy(part, part, s_in.at[0, j]).wait()
            pltpu.make_async_copy(dw2.at[j], dw2.at[j], s_in.at[1, j]).wait()


def _gradients(h, e, a, g):
    tokens, d = h.shape
    ff = e.shape[1]
    any_ = pl.BlockSpec(memory_space=pl.ANY)
    dma = pltpu.SemaphoreType.DMA
    return pl.pallas_call(
        _grad_kernel,
        out_shape=(jax.ShapeDtypeStruct((2, d, ff), F32), jax.ShapeDtypeStruct((2, ff, d), F32),
                   jax.ShapeDtypeStruct((d, TILE1), F32)),
        in_specs=[any_] * 4,
        out_specs=[any_] * 3,
        scratch_shapes=[
            pltpu.VMEM((DEPTH, KBLOCK, d), BF), pltpu.VMEM((DEPTH, KBLOCK, TILE1), BF),
            pltpu.VMEM((DEPTH, KBLOCK, TILE2), BF), pltpu.VMEM((SLOTS, d, TILE1), F32), pltpu.VMEM((SLOTS, TILE2, d), F32),
            dma((DEPTH,)), dma((DEPTH,)), dma((2, SLOTS)), dma((2, SLOTS)), dma((2, 2)),
        ],
        compiler_params=pltpu.CompilerParams(collective_id=1, has_side_effects=True, vmem_limit_bytes=67043328),
        cost_estimate=pl.CostEstimate(flops=4 * tokens * d * ff, bytes_accessed=4 * tokens * ff, transcendentals=0),
    )(h, e, a, g)


def _copy_kernel(a, b, a_out, b_out):
    a_out[...] = a[...]
    b_out[...] = b[...]


def _copies(dw1, dw2):
    _, d, ff = dw1.shape
    specs = [pl.BlockSpec((1, d // 8, ff), lambda j, i: (j, i, 0)), pl.BlockSpec((1, ff // 8, d), lambda j, i: (j, i, 0))]
    return pl.pallas_call(
        _copy_kernel,
        grid=(2, 8),
        out_shape=(jax.ShapeDtypeStruct(dw1.shape, F32), jax.ShapeDtypeStruct(dw2.shape, F32)),
        in_specs=specs,
        out_specs=specs,
        cost_estimate=pl.CostEstimate(flops=10 ** 11, bytes_accessed=32 * d * ff, transcendentals=0),
    )(dw1, dw2)


def solution(mesh):
    def flat(x, y, c):
        return y * 4 + 2 * x + c

    chips = [(x, y) for x in (0, 1) for y in (0, 1)]
    keep = [[(flat(x, y, j), flat(x, y, 1 - j)) for x, y in chips if (x + y) % 2 != j] for j in (0, 1)]
    swap = [[(flat(x, y, j), flat(x, 1 - y, (x + y) % 2)) for x, y in chips] for j in (0, 1)]

    def body(x, t, w1, w2):
        nm, tok, d = x.shape
        ff = w1.shape[-1]
        inv = 1.0 / (nm * tok * mesh.shape['dp'] * d)
        xs = x.reshape(nm * tok // ROWS, ROWS, d)
        ts = t.reshape(nm * tok // ROWS, ROWS, d)
        hb, _, ab, eb, gb, _, _, _, ls = _forward_backward(xs, ts, w1[0], w2[0], inv)
        n = hb.shape[0] * ROWS
        dw1, dw2, rest = _gradients(hb.reshape(n, d), eb.reshape(n, ff), ab.reshape(n, ff), gb.reshape(n, d))
        pp = lax.axis_index('pp')
        own = (pp // 2 + lax.axis_index('dp')) % 2 == pp % 2
        there = [lax.ppermute(rest, ('dp', 'pp'), swap[j]) for j in (0, 1)]
        here = [lax.ppermute(rest, ('dp', 'pp'), keep[j]) for j in (0, 1)]
        dw1, dw2 = _copies(dw1, dw2)
        for j in (0, 1):
            part = jnp.where(own, jnp.where(pp % 2 == j, rest, here[j]), there[j])
            dw1 = lax.dynamic_update_slice(dw1, part[None], (j, 0, ff - TILE1))
        loss = 0.5 * inv * jnp.sum(ls)
        return dw1[None], dw2[None], loss

    return jax.shard_map(body, mesh=mesh,
                         in_specs=(P(None, 'dp', None), P(None, 'dp', None), P('pp'), P('pp')),
                         out_specs=(P('pp'), P('pp'), P()), check_vma=False)
```

```python
import functools
import math
import jax
import jax.numpy as jnp
from jax import lax
from jax.experimental import pallas as pl
from jax.experimental.pallas import tpu as pltpu
from jax.sharding import PartitionSpec as P

MESH = pl.DeviceIdType.MESH
BF = jnp.bfloat16
F32 = jnp.float32
C = math.sqrt(2.0 / math.pi)
K3 = 0.044715
ROWS = 256
LAST_LAG = 4
BURST = 13
PAD = 256
SENDS = 4
PARTS = 4
KBLOCK = 1024
TILE1 = 512
TILE2 = 256
SLOTS = 4
DETOUR = 5
DEPTH = 4


def _gelu(u):
    z = u * (C + (C * K3) * (u * u))
    return (0.5 * u) * (1.0 + jnp.tanh(z))


def _dgelu_and_gelu(u):
    u2 = u * u
    th = jnp.tanh(u * (C + (C * K3) * u2))
    half = 0.5 * (1.0 + th)
    d = half + (0.5 * u) * (1.0 - th * th) * (C + (3.0 * C * K3) * u2)
    return d, u * half


def _place(q):
    xx = q // 4
    s = (q // 2) % 2
    return ((s + xx) % 2, 2 * xx + q % 2)


def _kernel(inv, x, t, w1, w2,
            hb, ub, ab, eb, gb, tb, wb1, wb2, ls,
            w1v, w2v, av, hr, lacc, ho, hv, tv, gl, gv, go, uo, ui, ao, eo,
            s_wr, s_ws, s_h, s_g, s_t, s_hl, s_tl, s_gl, s_ul, s_uw, s_aw, s_ew, s_hs, s_gs, s_glw, s_px, s_l, s_lx, s_wl):
    units, rows, d = hb.shape
    half_units = units // 2
    ff = ub.shape[2]
    dp = lax.axis_index('dp')
    pp = lax.axis_index('pp')
    xx = pp // 2
    c = pp % 2
    s_in = (xx + dp) % 2
    p = 4 * xx + 2 * s_in + c
    first = p == 0
    last = p == 7
    holder = c == s_in
    nxt = _place(jnp.minimum(p + 1, 7))
    prv = _place(jnp.maximum(p - 1, 0))
    lag = LAST_LAG + 6 * (7 - p) + 2 * ((7 - p) // 2)

    barrier = pltpu.get_barrier_semaphore()
    for i in range(1, 8):
        pl.semaphore_signal(barrier, inc=1, device_id=_place((p + i) % 8), device_id_type=MESH)
    pl.semaphore_wait(barrier, 7)

    def cut(ref, n):
        return ref.at[:, pl.ds(0, n)]

    def remote(src, dst, ss, rs, to):
        return pltpu.make_async_remote_copy(src_ref=src, dst_ref=dst, send_sem=ss, recv_sem=rs,
                                            device_id=to, device_id_type=MESH)

    def local(src, dst, sem):
        return pltpu.make_async_copy(src, dst, sem)

    sib = (dp, 2 * xx + 1 - c)

    @pl.when(holder)
    def _():
        local(w1.at[c], cut(w1v, ff), s_wr.at[0]).start()
        local(w2.at[c], cut(w2v, d), s_wr.at[1]).start()
        remote(w1.at[1 - c], wb1, s_ws.at[0], s_wr.at[0], sib).start()
        remote(w2.at[1 - c], wb2, s_ws.at[1], s_wr.at[1], sib).start()

    def push(src, dst, base, sem, to, k):
        remote(src.at[k], dst.at[base + k], s_px, sem.at[base + k], to).start()

    def push_all(src, dst, base, sem, to, n):
        def step(k, carry):
            push(src, dst, base, sem, to, k)
            return carry
        lax.fori_loop(0, n, step, 0)

    @pl.when(p == 1)
    def _():
        push_all(x, hb, 0, s_h, _place(0), half_units)

    @pl.when(p == 3)
    def _():
        push_all(x, hb, half_units, s_h, _place(0), half_units)

    @pl.when(p == 6)
    def _():
        push_all(t, tb, 0, s_t, _place(7), half_units)

    @pl.when(p == 4)
    def _():
        push_all(t, tb, half_units, s_t, _place(7), BURST)

    def paced_push(m):
        j = BURST + m // 2

        @pl.when((p == 4) & (j < half_units))
        def _():
            push(t, tb, half_units, s_t, _place(7), j)

    lacc[...] = jnp.zeros_like(lacc)
    local(w1.at[c], cut(w1v, ff), s_wr.at[0]).wait()

    @pl.when(jnp.logical_not(holder))
    def _():
        local(wb1, cut(w1v, ff), s_wl.at[0]).start()
    local(w2.at[c], cut(w2v, d), s_wr.at[1]).wait()

    @pl.when(jnp.logical_not(holder))
    def _():
        local(wb2, cut(w2v, d), s_wl.at[1]).start()
        local(wb1, cut(w1v, ff), s_wl.at[0]).wait()
        local(wb2, cut(w2v, d), s_wl.at[1]).wait()

    nt = (((1,), (1,)), ((), ()))
    nc, no = ff // PARTS, d // PARTS

    def f1(s, j):
        sl, so = slice(j * nc, (j + 1) * nc), slice(j * no, (j + 1) * no)
        u = jnp.dot(hv[s, :, :d], w1v[:, sl], preferred_element_type=F32).astype(BF)
        uo[s, :, sl] = u
        av[:, sl] = _gelu(u.astype(F32)).astype(BF)
        hr[:, so] = hv[s, :, so]

    def f2(k, s, j):
        sl = slice(j * no, (j + 1) * no)
        acc = jnp.dot(av[:, :ff], w2v[:, sl], preferred_element_type=F32)
        y = (hr[:, sl].astype(F32) + acc).astype(BF)
        ho[k % SENDS, :, sl] = y
        r = y.astype(F32) - tv[s, :, sl].astype(F32)
        gl[s, :, sl] = (r * inv).astype(BF)
        lacc[:, sl] += jnp.sum((r * r).reshape(rows // 8, 8, no), axis=0)

    def b1(s, j):
        sl = slice(j * nc, (j + 1) * nc)
        q = lax.dot_general(gv[s, :, :d], w2v[sl, :d], nt, preferred_element_type=F32)
        dg, a = _dgelu_and_gelu(ui[s, :, sl].astype(F32))
        ao[s, :, sl] = a.astype(BF)
        eo[s, :, sl] = (dg * q).astype(BF)

    def b2(s, j):
        sl = slice(j * no, (j + 1) * no)
        acc = lax.dot_general(eo[s, :, :ff], w1v[sl, :ff], nt, preferred_element_type=F32)
        go[s, :, sl] = (gv[s, :, sl].astype(F32) + acc).astype(BF)

    def h_load(k, s):
        return local(hb.at[k], cut(hv.at[s], d), s_hl.at[s])

    def t_load(k, s):
        return local(tb.at[k], cut(tv.at[s], d), s_tl.at[s])

    def g_load(m, s):
        return local(gb.at[m], cut(gv.at[s], d), s_gl.at[s])

    def u_load(m, s):
        return local(ub.at[m], cut(ui.at[s], ff), s_ul.at[s])

    def u_write(k, s):
        return local(cut(uo.at[s], ff), ub.at[k], s_uw.at[s])

    def a_write(m, s):
        return local(cut(ao.at[s], ff), ab.at[m], s_aw.at[s])

    def e_write(m, s):
        return local(cut(eo.at[s], ff), eb.at[m], s_ew.at[s])

    def gl_write(k, s):
        return local(cut(gl.at[s], d), gb.at[k], s_glw.at[s])

    def h_send(k, s):
        return remote(ho.at[k % SENDS, :, pl.ds(0, d)], hb.at[k], s_hs.at[k % SENDS], s_h.at[k], nxt)

    def g_send(m, s):
        return remote(cut(go.at[s], d), gb.at[m], s_gs.at[s], s_g.at[m], prv)

    def fetch_h(k, s):
        local(hb.at[k], hb.at[k], s_h.at[k]).wait()
        h_load(k, s).start()

    def fetch_t(k, s):
        @pl.when(last)
        def _():
            local(tb.at[k], tb.at[k], s_t.at[k]).wait()
            t_load(k, s).start()

    def fetch_g(m, s):
        @pl.when(jnp.logical_not(last))
        def _():
            local(gb.at[m], gb.at[m], s_g.at[m]).wait()
        g_load(m, s).start()

    def wait_t(k, s):
        @pl.when(last)
        def _():
            t_load(k, s).wait()

    def wait_gl(k, s):
        @pl.when(last & (k >= 0))
        def _():
            gl_write(k, s).wait()

    def wait_h_send(k, s):
        @pl.when(jnp.logical_not(last) & (k >= 0))
        def _():
            h_send(k, s).wait_send()

    def wait_b_outputs(m, s):
        a_write(m, s).wait()
        e_write(m, s).wait()

        @pl.when(p > 0)
        def _():
            g_send(m, s).wait_send()

    def put_f(k, s):
        @pl.when(last)
        def _():
            gl_write(k, s).start()

        @pl.when(jnp.logical_not(last))
        def _():
            h_send(k, s).start()

    def put_b(m, s):
        @pl.when(p > 0)
        def _():
            g_send(m, s).start()

    def warm(k, carry):
        s = k % 2
        h_load(k, s).wait()
        wait_t(k, s)

        @pl.when(k >= 2)
        def _():
            u_write(k - 2, s).wait()
        wait_gl(k - 2, s)
        wait_h_send(k - SENDS, s)
        for j in range(PARTS):
            f1(s, j)
        for j in range(PARTS):
            f2(k, s, j)
        put_f(k, s)
        u_write(k, s).start()
        fetch_h(k + 1, 1 - s)
        fetch_t(k + 1, 1 - s)
        return carry

    def steady(i, carry):
        for s in (0, 1):
            m = 2 * i + s
            k = lag + m
            if s == 0:
                paced_push(m)
            h_load(k, s).wait()
            wait_t(k - 1, 1 - s)
            g_load(m, s).wait()
            u_load(m, s).wait()
            u_write(k - 2, s).wait()
            wait_gl(k - 3, 1 - s)
            wait_h_send(k - 1 - SENDS, 1 - s)

            @pl.when(m >= 2)
            def _():
                wait_b_outputs(m - 2, s)
            u_load(m + 1, 1 - s).start()

            @pl.when(k + 1 < units)
            def _():
                fetch_h(k + 1, 1 - s)
            fetch_t(k, s)
            fetch_g(m + 1, 1 - s)
            for j in range(PARTS):
                f2(k - 1, 1 - s, j)
                b1(s, j)
            for j in range(PARTS):
                b2(s, j)
                f1(s, j)
            put_f(k - 1, 1 - s)
            put_b(m, s)
            u_write(k, s).start()
            e_write(m, s).start()
            a_write(m, s).start()
        return carry

    def cool(i, carry):
        m = units - lag + i
        s = m % 2
        g_load(m, s).wait()
        u_load(m, s).wait()

        @pl.when(m >= 2)
        def _():
            wait_b_outputs(m - 2, s)

        @pl.when(m + 1 < units)
        def _():
            u_load(m + 1, 1 - s).start()
        for j in range(PARTS):
            b1(s, j)
        for j in range(PARTS):
            b2(s, j)
        put_b(m, s)
        e_write(m, s).start()
        a_write(m, s).start()

        @pl.when(m + 1 < units)
        def _():
            fetch_g(m + 1, 1 - s)
        return carry

    fetch_h(0, 0)
    fetch_t(0, 0)
    lax.fori_loop(0, lag - 1, warm, 0)

    h_load(lag - 1, 1).wait()
    u_write(lag - 3, 1).wait()
    for j in range(PARTS):
        f1(1, j)
    u_write(lag - 1, 1).start()
    fetch_h(lag, 0)
    u_load(0, 0).start()
    fetch_g(0, 0)
    lax.fori_loop(0, (units - lag) // 2, steady, 0)

    wait_t(units - 1, 1)
    wait_gl(units - 3, 1)
    wait_h_send(units - 1 - SENDS, 1)
    for j in range(PARTS):
        f2(units - 1, 1, j)
    put_f(units - 1, 1)
    u_write(units - 2, 0).wait()
    u_write(units - 1, 1).wait()
    wait_gl(units - 2, 0)
    wait_gl(units - 1, 1)

    @pl.when(last)
    def _():
        local(lacc, ls, s_l).start()
        for i in range(7):
            remote(lacc, ls, s_lx.at[i], s_l, _place(i)).start()

    lax.fori_loop(0, lag, cool, 0)
    for i in range(SENDS):
        wait_h_send(units - SENDS + i, i % 2)
    wait_b_outputs(units - 2, 0)
    wait_b_outputs(units - 1, 1)
    local(lacc, ls, s_l).wait()

    @pl.when(last)
    def _():
        for i in range(7):
            remote(lacc, ls, s_lx.at[i], s_l, _place(i)).wait_send()

    @pl.when(holder)
    def _():
        remote(w1.at[1 - c], wb1, s_ws.at[0], s_wr.at[0], sib).wait_send()
        remote(w2.at[1 - c], wb2, s_ws.at[1], s_wr.at[1], sib).wait_send()

    @pl.when((p == 1) | (p == 3))
    def _():
        remote(x, hb.at[pl.ds(0, half_units)], s_px, s_h.at[0], _place(0)).wait_send()

    @pl.when((p == 4) | (p == 6))
    def _():
        remote(t, tb.at[pl.ds(0, half_units)], s_px, s_t.at[0], _place(7)).wait_send()


def _forward_backward(x, t, w1, w2, inv):
    half_units, rows, d = x.shape
    units = 2 * half_units
    ff = w1.shape[-1]
    any_ = pl.BlockSpec(memory_space=pl.ANY)
    dw, fw = d + PAD, ff + PAD
    small = [pltpu.VMEM((2, rows, dw), BF)]
    big = [pltpu.VMEM((2, rows, fw), BF)]
    dma = pltpu.SemaphoreType.DMA
    narrow = jax.ShapeDtypeStruct((units, rows, d), BF)
    wide = jax.ShapeDtypeStruct((units, rows, ff), BF)

    def kern(*refs):
        _kernel(inv, *refs)

    flops = 8 * units * rows * d * ff
    return pl.pallas_call(
        kern,
        out_shape=(narrow, wide, wide, wide, narrow, narrow, jax.ShapeDtypeStruct((d, ff), BF),
                   jax.ShapeDtypeStruct((ff, d), BF), jax.ShapeDtypeStruct((8, d), F32)),
        in_specs=[any_] * 4,
        out_specs=[any_] * 9,
        scratch_shapes=[
            pltpu.VMEM((d, fw), BF), pltpu.VMEM((ff, dw), BF), pltpu.VMEM((rows, fw), BF),
            pltpu.VMEM((rows, dw), BF), pltpu.VMEM((8, d), F32), pltpu.VMEM((SENDS, rows, dw), BF),
            *(small * 5), *(big * 4),
            dma((2,)), dma((2,)), dma((units,)), dma((units,)), dma((units,)),
            dma((2,)), dma((2,)), dma((2,)), dma((2,)), dma((2,)), dma((2,)), dma((2,)),
            dma((SENDS,)), dma((2,)), dma((2,)), dma(()), dma(()), dma((7,)), dma((2,)),
        ],
        compiler_params=pltpu.CompilerParams(collective_id=0, has_side_effects=True, vmem_limit_bytes=67043328),
        cost_estimate=pl.CostEstimate(flops=flops, bytes_accessed=10 * units * rows * ff, transcendentals=0),
    )(x, t, w1, w2)


def _grad_kernel(h, e, a, g, dw1, dw2, rest, via1, via2, narrow, wide1, wide2, acc1, acc2,
                 s_n, s_w, s_keep, s_send, s_in, s_via, s_relay):
    tokens, d = h.shape
    ff = e.shape[1]
    blocks = tokens // KBLOCK
    dp = lax.axis_index('dp')
    pp = lax.axis_index('pp')
    xx = pp // 2
    c = pp % 2
    side = (xx + dp) % 2
    own = c == side
    here = (dp, 2 * xx + side)
    there = (1 - dp, 2 * xx + side)

    barrier = pltpu.get_barrier_semaphore()
    for i in range(1, 4):
        to = ((dp + i // 2) % 2, 2 * xx + (c + i) % 2)
        pl.semaphore_signal(barrier, inc=1, device_id=to, device_id_type=MESH)
    @pl.when(xx == 1)
    def _():
        pl.semaphore_signal(barrier, inc=1, device_id=(dp, c), device_id_type=MESH)
        pl.semaphore_wait(barrier, 3)

    @pl.when(xx == 0)
    def _():
        pl.semaphore_wait(barrier, 4)

    def phase(thin, fat, wide, acc, out, cols, arr):
        tile = wide.shape[-1]
        tiles = ff // tile
        sent = tiles - 1 if cols else tiles

        def load(t, s):
            k = pl.multiple_of((t % blocks) * KBLOCK, KBLOCK)
            n = pl.multiple_of((t // blocks) * tile, tile)
            return (pltpu.make_async_copy(thin.at[pl.ds(k, KBLOCK)], narrow.at[s], s_n.at[s]),
                    pltpu.make_async_copy(fat.at[pl.ds(k, KBLOCK), pl.ds(n, tile)], wide.at[s], s_w.at[s]))

        def place(i):
            n = pl.multiple_of(i * tile, tile)
            return out.at[c, :, pl.ds(n, tile)] if cols else out.at[c, pl.ds(n, tile)]

        def keep_local(i, slot):
            return pltpu.make_async_copy(acc.at[slot], place(i), s_keep.at[arr, slot])

        def keep_remote(i, slot):
            return pltpu.make_async_remote_copy(acc.at[slot], place(i), s_keep.at[arr, slot], s_in.at[arr, c],
                                                device_id=here, device_id_type=MESH)

        def send(i, slot):
            return pltpu.make_async_remote_copy(acc.at[slot], place(i), s_send.at[arr, slot], s_in.at[arr, c],
                                                device_id=there, device_id_type=MESH)

        def detour(slot):
            return pltpu.make_async_remote_copy(acc.at[slot], via1, s_send.at[arr, slot], s_via.at[0],
                                                device_id=(dp, 2 + c), device_id_type=MESH)

        def rest_local(slot):
            return pltpu.make_async_copy(acc.at[slot], rest, s_keep.at[arr, slot])

        def drain(i, slot):
            send(i, slot).wait_send()

            @pl.when(jnp.logical_not(own))
            def _():
                keep_remote(i, slot).wait_send()

            @pl.when(own)
            def _():
                keep_local(i, slot).wait()

        for ahead in range(DEPTH - 1):
            for cp in load(ahead, ahead):
                cp.start()

        def step(t, carry):
            s = t % DEPTH
            i = t // blocks
            k = t % blocks
            slot = i % SLOTS

            @pl.when(k == 0)
            def _():
                @pl.when(i >= SLOTS)
                def _():
                    drain(i - SLOTS, slot)
                acc[slot] = jnp.zeros(acc.shape[1:], F32)
            for cp in load(t, s):
                cp.wait()

            @pl.when(t + DEPTH - 1 < tiles * blocks)
            def _():
                for cp in load(t + DEPTH - 1, (t + DEPTH - 1) % DEPTH):
                    cp.start()
            lhs, rhs = (narrow, wide) if cols else (wide, narrow)
            for q in range(acc.shape[1] // 256):
                rows = slice(q * 256, (q + 1) * 256)
                acc[slot, rows, :] += lax.dot_general(lhs[s, :, rows], rhs[s], (((0,), (0,)), ((), ())),
                                                      preferred_element_type=F32)

            if sent < tiles:
                @pl.when(t == tiles * blocks - 1)
                def _():
                    rest_local(slot).start()

            @pl.when((k == blocks - 1) & (i < sent))
            def _():
                if cols:
                    send(i, slot).start()
                else:
                    around = (xx == 0) & (i == DETOUR)

                    @pl.when(jnp.logical_not(around))
                    def _():
                        send(i, slot).start()

                    @pl.when(around)
                    def _():
                        detour(slot).start()

                @pl.when(own)
                def _():
                    keep_local(i, slot).start()

                @pl.when(jnp.logical_not(own))
                def _():
                    keep_remote(i, slot).start()
            return carry

        lax.fori_loop(0, tiles * blocks, step, 0)
        for i in range(tiles - SLOTS, sent):
            late.append(functools.partial(drain, i, i % SLOTS))
        if sent < tiles:
            late.append(lambda: rest_local((tiles - 1) % SLOTS).wait())

    late = []
    relay1 = pltpu.make_async_remote_copy(via1, via2, s_relay.at[0], s_via.at[1],
                                          device_id=(1 - dp, 2 + c), device_id_type=MESH)
    relay2 = pltpu.make_async_remote_copy(via2, dw2.at[c, pl.ds(DETOUR * TILE2, TILE2)], s_relay.at[1], s_in.at[1, c],
                                          device_id=(dp, 1 - dp), device_id_type=MESH)
    phase(g, a, wide2, acc2, dw2, False, 1)

    @pl.when(xx == 1)
    def _():
        pltpu.make_async_copy(via1, via1, s_via.at[0]).wait()
        relay1.start()
    phase(h, e, wide1, acc1, dw1, True, 0)

    @pl.when(xx == 1)
    def _():
        pltpu.make_async_copy(via2, via2, s_via.at[1]).wait()
        relay2.start()
    for wait in late:
        wait()

    @pl.when(xx == 1)
    def _():
        relay1.wait_send()
        relay2.wait_send()

    for j in (0, 1):
        @pl.when(jnp.logical_not(own) | (c != j))
        def _():
            part = dw1.at[j, :, pl.ds(0, ff - TILE1)]
            pltpu.make_async_copy(part, part, s_in.at[0, j]).wait()
            pltpu.make_async_copy(dw2.at[j], dw2.at[j], s_in.at[1, j]).wait()


def _gradients(h, e, a, g):
    tokens, d = h.shape
    ff = e.shape[1]
    any_ = pl.BlockSpec(memory_space=pl.ANY)
    dma = pltpu.SemaphoreType.DMA
    return pl.pallas_call(
        _grad_kernel,
        out_shape=(jax.ShapeDtypeStruct((2, d, ff), F32), jax.ShapeDtypeStruct((2, ff, d), F32),
                   jax.ShapeDtypeStruct((d, TILE1), F32),
                   jax.ShapeDtypeStruct((TILE2, d), F32), jax.ShapeDtypeStruct((TILE2, d), F32)),
        in_specs=[any_] * 4,
        out_specs=[any_] * 5,
        scratch_shapes=[
            pltpu.VMEM((DEPTH, KBLOCK, d), BF), pltpu.VMEM((DEPTH, KBLOCK, TILE1), BF),
            pltpu.VMEM((DEPTH, KBLOCK, TILE2), BF), pltpu.VMEM((SLOTS, d, TILE1), F32), pltpu.VMEM((SLOTS, TILE2, d), F32),
            dma((DEPTH,)), dma((DEPTH,)), dma((2, SLOTS)), dma((2, SLOTS)), dma((2, 2)), dma((2,)), dma((2,)),
        ],
        compiler_params=pltpu.CompilerParams(collective_id=1, has_side_effects=True, vmem_limit_bytes=67043328),
        cost_estimate=pl.CostEstimate(flops=4 * tokens * d * ff, bytes_accessed=4 * tokens * ff, transcendentals=0),
    )(h, e, a, g)


def _copy_kernel(a, b, a_out, b_out):
    a_out[...] = a[...]
    b_out[...] = b[...]


def _copies(dw1, dw2):
    _, d, ff = dw1.shape
    specs = [pl.BlockSpec((1, d // 8, ff), lambda j, i: (j, i, 0)), pl.BlockSpec((1, ff // 8, d), lambda j, i: (j, i, 0))]
    return pl.pallas_call(
        _copy_kernel,
        grid=(2, 8),
        out_shape=(jax.ShapeDtypeStruct(dw1.shape, F32), jax.ShapeDtypeStruct(dw2.shape, F32)),
        in_specs=specs,
        out_specs=specs,
        cost_estimate=pl.CostEstimate(flops=10 ** 11, bytes_accessed=32 * d * ff, transcendentals=0),
    )(dw1, dw2)


def solution(mesh):
    def flat(x, y, c):
        return y * 4 + 2 * x + c

    chips = [(x, y) for x in (0, 1) for y in (0, 1)]
    keep = [[(flat(x, y, j), flat(x, y, 1 - j)) for x, y in chips if (x + y) % 2 != j] for j in (0, 1)]
    swap = [[(flat(x, y, j), flat(x, 1 - y, (x + y) % 2)) for x, y in chips] for j in (0, 1)]

    def body(x, t, w1, w2):
        nm, tok, d = x.shape
        ff = w1.shape[-1]
        inv = 1.0 / (nm * tok * mesh.shape['dp'] * d)
        xs = x.reshape(nm * tok // ROWS, ROWS, d)
        ts = t.reshape(nm * tok // ROWS, ROWS, d)
        hb, _, ab, eb, gb, _, _, _, ls = _forward_backward(xs, ts, w1[0], w2[0], inv)
        n = hb.shape[0] * ROWS
        dw1, dw2, rest, _, _ = _gradients(hb.reshape(n, d), eb.reshape(n, ff), ab.reshape(n, ff), gb.reshape(n, d))
        pp = lax.axis_index('pp')
        own = (pp // 2 + lax.axis_index('dp')) % 2 == pp % 2
        there = [lax.ppermute(rest, ('dp', 'pp'), swap[j]) for j in (0, 1)]
        here = [lax.ppermute(rest, ('dp', 'pp'), keep[j]) for j in (0, 1)]
        dw1, dw2 = _copies(dw1, dw2)
        for j in (0, 1):
            part = jnp.where(own, jnp.where(pp % 2 == j, rest, here[j]), there[j])
            dw1 = lax.dynamic_update_slice(dw1, part[None], (j, 0, ff - TILE1))
        loss = 0.5 * inv * jnp.sum(ls)
        return dw1[None], dw2[None], loss

    return jax.shard_map(body, mesh=mesh,
                         in_specs=(P(None, 'dp', None), P(None, 'dp', None), P('pp'), P('pp')),
                         out_specs=(P('pp'), P('pp'), P()), check_vma=False)
```

```python
import functools
import math
import jax
import jax.numpy as jnp
from jax import lax
from jax.experimental import pallas as pl
from jax.experimental.pallas import tpu as pltpu
from jax.sharding import PartitionSpec as P

MESH = pl.DeviceIdType.MESH
BF = jnp.bfloat16
F32 = jnp.float32
C = math.sqrt(2.0 / math.pi)
K3 = 0.044715
ROWS = 256
LAST_LAG = 4
BURST = 13
PAD = 256
SENDS = 4
PARTS = 4
KBLOCK = 1024
TILE1 = 512
TILE2 = 256
SLOTS = 4
DETOUR = 5
DEPTH = 4


def _gelu(u):
    z = u * (C + (C * K3) * (u * u))
    return (0.5 * u) * (1.0 + jnp.tanh(z))


def _dgelu_and_gelu(u):
    u2 = u * u
    th = jnp.tanh(u * (C + (C * K3) * u2))
    half = 0.5 * (1.0 + th)
    d = half + (0.5 * u) * (1.0 - th * th) * (C + (3.0 * C * K3) * u2)
    return d, u * half


def _place(q):
    xx = q // 4
    s = (q // 2) % 2
    return ((s + xx) % 2, 2 * xx + q % 2)


def _kernel(inv, x, t, w1, w2,
            hb, ub, ab, eb, gb, tb, wb1, wb2, ls,
            w1v, w2v, av, hr, lacc, ho, hv, tv, gl, gv, go, uo, ui, ao, eo,
            s_wr, s_ws, s_h, s_g, s_t, s_hl, s_tl, s_gl, s_ul, s_uw, s_aw, s_ew, s_hs, s_gs, s_glw, s_px, s_l, s_lx, s_wl):
    units, rows, d = hb.shape
    half_units = units // 2
    ff = ub.shape[2]
    dp = lax.axis_index('dp')
    pp = lax.axis_index('pp')
    xx = pp // 2
    c = pp % 2
    s_in = (xx + dp) % 2
    p = 4 * xx + 2 * s_in + c
    first = p == 0
    last = p == 7
    holder = c == s_in
    nxt = _place(jnp.minimum(p + 1, 7))
    prv = _place(jnp.maximum(p - 1, 0))
    lag = LAST_LAG + 6 * (7 - p) + 2 * ((7 - p) // 2)

    barrier = pltpu.get_barrier_semaphore()
    for i in range(1, 8):
        pl.semaphore_signal(barrier, inc=1, device_id=_place((p + i) % 8), device_id_type=MESH)
    pl.semaphore_wait(barrier, 7)

    def cut(ref, n):
        return ref.at[:, pl.ds(0, n)]

    def remote(src, dst, ss, rs, to):
        return pltpu.make_async_remote_copy(src_ref=src, dst_ref=dst, send_sem=ss, recv_sem=rs,
                                            device_id=to, device_id_type=MESH)

    def local(src, dst, sem):
        return pltpu.make_async_copy(src, dst, sem)

    sib = (dp, 2 * xx + 1 - c)

    @pl.when(holder)
    def _():
        local(w1.at[c], cut(w1v, ff), s_wr.at[0]).start()
        local(w2.at[c], cut(w2v, d), s_wr.at[1]).start()
        remote(w1.at[1 - c], wb1, s_ws.at[0], s_wr.at[0], sib).start()
        remote(w2.at[1 - c], wb2, s_ws.at[1], s_wr.at[1], sib).start()

    def push(src, dst, base, sem, to, k):
        remote(src.at[k], dst.at[base + k], s_px, sem.at[base + k], to).start()

    def push_all(src, dst, base, sem, to, n):
        def step(k, carry):
            push(src, dst, base, sem, to, k)
            return carry
        lax.fori_loop(0, n, step, 0)

    @pl.when(p == 1)
    def _():
        push_all(x, hb, 0, s_h, _place(0), half_units)

    @pl.when(p == 3)
    def _():
        push_all(x, hb, half_units, s_h, _place(0), half_units)

    @pl.when(p == 6)
    def _():
        push_all(t, tb, 0, s_t, _place(7), half_units)

    @pl.when(p == 4)
    def _():
        push_all(t, tb, half_units, s_t, _place(7), BURST)

    def paced_push(m):
        j = BURST + m // 2

        @pl.when((p == 4) & (j < half_units))
        def _():
            push(t, tb, half_units, s_t, _place(7), j)

    lacc[...] = jnp.zeros_like(lacc)
    local(w1.at[c], cut(w1v, ff), s_wr.at[0]).wait()

    @pl.when(jnp.logical_not(holder))
    def _():
        local(wb1, cut(w1v, ff), s_wl.at[0]).start()
    local(w2.at[c], cut(w2v, d), s_wr.at[1]).wait()

    @pl.when(jnp.logical_not(holder))
    def _():
        local(wb2, cut(w2v, d), s_wl.at[1]).start()
        local(wb1, cut(w1v, ff), s_wl.at[0]).wait()
        local(wb2, cut(w2v, d), s_wl.at[1]).wait()

    nt = (((1,), (1,)), ((), ()))
    nc, no = ff // PARTS, d // PARTS

    def f1(s, j):
        sl, so = slice(j * nc, (j + 1) * nc), slice(j * no, (j + 1) * no)
        u = jnp.dot(hv[s, :, :d], w1v[:, sl], preferred_element_type=F32).astype(BF)
        uo[s, :, sl] = u
        av[:, sl] = _gelu(u.astype(F32)).astype(BF)
        hr[:, so] = hv[s, :, so]

    def f2(k, s, j):
        sl = slice(j * no, (j + 1) * no)
        acc = jnp.dot(av[:, :ff], w2v[:, sl], preferred_element_type=F32)
        y = (hr[:, sl].astype(F32) + acc).astype(BF)
        ho[k % SENDS, :, sl] = y
        r = y.astype(F32) - tv[s, :, sl].astype(F32)
        gl[s, :, sl] = (r * inv).astype(BF)
        lacc[:, sl] += jnp.sum((r * r).reshape(rows // 8, 8, no), axis=0)

    def b1(s, j):
        sl = slice(j * nc, (j + 1) * nc)
        q = lax.dot_general(gv[s, :, :d], w2v[sl, :d], nt, preferred_element_type=F32)
        dg, a = _dgelu_and_gelu(ui[s, :, sl].astype(F32))
        ao[s, :, sl] = a.astype(BF)
        eo[s, :, sl] = (dg * q).astype(BF)

    def b2(s, j):
        sl = slice(j * no, (j + 1) * no)
        acc = lax.dot_general(eo[s, :, :ff], w1v[sl, :ff], nt, preferred_element_type=F32)
        go[s, :, sl] = (gv[s, :, sl].astype(F32) + acc).astype(BF)

    def h_load(k, s):
        return local(hb.at[k], cut(hv.at[s], d), s_hl.at[s])

    def t_load(k, s):
        return local(tb.at[k], cut(tv.at[s], d), s_tl.at[s])

    def g_load(m, s):
        return local(gb.at[m], cut(gv.at[s], d), s_gl.at[s])

    def u_load(m, s):
        return local(ub.at[m], cut(ui.at[s], ff), s_ul.at[s])

    def u_write(k, s):
        return local(cut(uo.at[s], ff), ub.at[k], s_uw.at[s])

    def a_write(m, s):
        return local(cut(ao.at[s], ff), ab.at[m], s_aw.at[s])

    def e_write(m, s):
        return local(cut(eo.at[s], ff), eb.at[m], s_ew.at[s])

    def gl_write(k, s):
        return local(cut(gl.at[s], d), gb.at[k], s_glw.at[s])

    def h_send(k, s):
        return remote(ho.at[k % SENDS, :, pl.ds(0, d)], hb.at[k], s_hs.at[k % SENDS], s_h.at[k], nxt)

    def g_send(m, s):
        return remote(cut(go.at[s], d), gb.at[m], s_gs.at[s], s_g.at[m], prv)

    def fetch_h(k, s):
        local(hb.at[k], hb.at[k], s_h.at[k]).wait()
        h_load(k, s).start()

    def fetch_t(k, s):
        @pl.when(last)
        def _():
            local(tb.at[k], tb.at[k], s_t.at[k]).wait()
            t_load(k, s).start()

    def fetch_g(m, s):
        @pl.when(jnp.logical_not(last))
        def _():
            local(gb.at[m], gb.at[m], s_g.at[m]).wait()
        g_load(m, s).start()

    def wait_t(k, s):
        @pl.when(last)
        def _():
            t_load(k, s).wait()

    def wait_gl(k, s):
        @pl.when(last & (k >= 0))
        def _():
            gl_write(k, s).wait()

    def wait_h_send(k, s):
        @pl.when(jnp.logical_not(last) & (k >= 0))
        def _():
            h_send(k, s).wait_send()

    def wait_b_outputs(m, s):
        a_write(m, s).wait()
        e_write(m, s).wait()

        @pl.when(p > 0)
        def _():
            g_send(m, s).wait_send()

    def put_f(k, s):
        @pl.when(last)
        def _():
            gl_write(k, s).start()

        @pl.when(jnp.logical_not(last))
        def _():
            h_send(k, s).start()

    def put_b(m, s):
        @pl.when(p > 0)
        def _():
            g_send(m, s).start()

    def warm(k, carry):
        s = k % 2
        h_load(k, s).wait()
        wait_t(k, s)

        @pl.when(k >= 2)
        def _():
            u_write(k - 2, s).wait()
        wait_gl(k - 2, s)
        wait_h_send(k - SENDS, s)
        for j in range(PARTS):
            f1(s, j)
        for j in range(PARTS):
            f2(k, s, j)
        put_f(k, s)
        u_write(k, s).start()
        fetch_h(k + 1, 1 - s)
        fetch_t(k + 1, 1 - s)
        return carry

    def steady(i, carry):
        for s in (0, 1):
            m = 2 * i + s
            k = lag + m
            if s == 0:
                paced_push(m)
            h_load(k, s).wait()
            wait_t(k - 1, 1 - s)
            g_load(m, s).wait()
            u_load(m, s).wait()
            u_write(k - 2, s).wait()
            wait_gl(k - 3, 1 - s)
            wait_h_send(k - 1 - SENDS, 1 - s)

            @pl.when(m >= 2)
            def _():
                wait_b_outputs(m - 2, s)
            u_load(m + 1, 1 - s).start()

            @pl.when(k + 1 < units)
            def _():
                fetch_h(k + 1, 1 - s)
            fetch_t(k, s)
            fetch_g(m + 1, 1 - s)
            for j in range(PARTS):
                f2(k - 1, 1 - s, j)
                b1(s, j)
            for j in range(PARTS):
                b2(s, j)
                f1(s, j)
            put_f(k - 1, 1 - s)
            put_b(m, s)
            u_write(k, s).start()
            e_write(m, s).start()
            a_write(m, s).start()
        return carry

    def cool(i, carry):
        m = units - lag + i
        s = m % 2
        g_load(m, s).wait()
        u_load(m, s).wait()

        @pl.when(m >= 2)
        def _():
            wait_b_outputs(m - 2, s)

        @pl.when(m + 1 < units)
        def _():
            u_load(m + 1, 1 - s).start()
        for j in range(PARTS):
            b1(s, j)
        for j in range(PARTS):
            b2(s, j)
        put_b(m, s)
        e_write(m, s).start()
        a_write(m, s).start()

        @pl.when(m + 1 < units)
        def _():
            fetch_g(m + 1, 1 - s)
        return carry

    fetch_h(0, 0)
    fetch_t(0, 0)
    lax.fori_loop(0, lag - 1, warm, 0)

    h_load(lag - 1, 1).wait()
    u_write(lag - 3, 1).wait()
    for j in range(PARTS):
        f1(1, j)
    u_write(lag - 1, 1).start()
    fetch_h(lag, 0)
    u_load(0, 0).start()
    fetch_g(0, 0)
    lax.fori_loop(0, (units - lag) // 2, steady, 0)

    wait_t(units - 1, 1)
    wait_gl(units - 3, 1)
    wait_h_send(units - 1 - SENDS, 1)
    for j in range(PARTS):
        f2(units - 1, 1, j)
    put_f(units - 1, 1)
    u_write(units - 2, 0).wait()
    u_write(units - 1, 1).wait()
    wait_gl(units - 2, 0)
    wait_gl(units - 1, 1)

    @pl.when(last)
    def _():
        local(lacc, ls, s_l).start()
        for i in range(7):
            remote(lacc, ls, s_lx.at[i], s_l, _place(i)).start()

    lax.fori_loop(0, lag, cool, 0)
    for i in range(SENDS):
        wait_h_send(units - SENDS + i, i % 2)
    wait_b_outputs(units - 2, 0)
    wait_b_outputs(units - 1, 1)
    local(lacc, ls, s_l).wait()

    @pl.when(last)
    def _():
        for i in range(7):
            remote(lacc, ls, s_lx.at[i], s_l, _place(i)).wait_send()

    @pl.when(holder)
    def _():
        remote(w1.at[1 - c], wb1, s_ws.at[0], s_wr.at[0], sib).wait_send()
        remote(w2.at[1 - c], wb2, s_ws.at[1], s_wr.at[1], sib).wait_send()

    @pl.when((p == 1) | (p == 3))
    def _():
        remote(x, hb.at[pl.ds(0, half_units)], s_px, s_h.at[0], _place(0)).wait_send()

    @pl.when((p == 4) | (p == 6))
    def _():
        remote(t, tb.at[pl.ds(0, half_units)], s_px, s_t.at[0], _place(7)).wait_send()


def _forward_backward(x, t, w1, w2, inv):
    half_units, rows, d = x.shape
    units = 2 * half_units
    ff = w1.shape[-1]
    any_ = pl.BlockSpec(memory_space=pl.ANY)
    dw, fw = d + PAD, ff + PAD
    small = [pltpu.VMEM((2, rows, dw), BF)]
    big = [pltpu.VMEM((2, rows, fw), BF)]
    dma = pltpu.SemaphoreType.DMA
    narrow = jax.ShapeDtypeStruct((units, rows, d), BF)
    wide = jax.ShapeDtypeStruct((units, rows, ff), BF)

    def kern(*refs):
        _kernel(inv, *refs)

    flops = 8 * units * rows * d * ff
    return pl.pallas_call(
        kern,
        out_shape=(narrow, wide, wide, wide, narrow, narrow, jax.ShapeDtypeStruct((d, ff), BF),
                   jax.ShapeDtypeStruct((ff, d), BF), jax.ShapeDtypeStruct((8, d), F32)),
        in_specs=[any_] * 4,
        out_specs=[any_] * 9,
        scratch_shapes=[
            pltpu.VMEM((d, fw), BF), pltpu.VMEM((ff, dw), BF), pltpu.VMEM((rows, fw), BF),
            pltpu.VMEM((rows, dw), BF), pltpu.VMEM((8, d), F32), pltpu.VMEM((SENDS, rows, dw), BF),
            *(small * 5), *(big * 4),
            dma((2,)), dma((2,)), dma((units,)), dma((units,)), dma((units,)),
            dma((2,)), dma((2,)), dma((2,)), dma((2,)), dma((2,)), dma((2,)), dma((2,)),
            dma((SENDS,)), dma((2,)), dma((2,)), dma(()), dma(()), dma((7,)), dma((2,)),
        ],
        compiler_params=pltpu.CompilerParams(collective_id=0, has_side_effects=True, vmem_limit_bytes=67043328),
        cost_estimate=pl.CostEstimate(flops=flops, bytes_accessed=10 * units * rows * ff, transcendentals=0),
    )(x, t, w1, w2)


def _grad_kernel(h, e, a, g, dw1, dw2, rest, via1, via2, narrow, wide1, wide2, acc1, acc2,
                 s_n, s_w, s_keep, s_send, s_in, s_via, s_relay):
    tokens, d = h.shape
    ff = e.shape[1]
    blocks = tokens // KBLOCK
    dp = lax.axis_index('dp')
    pp = lax.axis_index('pp')
    xx = pp // 2
    c = pp % 2
    side = (xx + dp) % 2
    own = c == side
    here = (dp, 2 * xx + side)
    there = (1 - dp, 2 * xx + side)

    barrier = pltpu.get_barrier_semaphore()
    for i in range(1, 4):
        to = ((dp + i // 2) % 2, 2 * xx + (c + i) % 2)
        pl.semaphore_signal(barrier, inc=1, device_id=to, device_id_type=MESH)
    @pl.when(xx == 1)
    def _():
        pl.semaphore_signal(barrier, inc=1, device_id=(dp, c), device_id_type=MESH)
        pl.semaphore_wait(barrier, 3)

    @pl.when(xx == 0)
    def _():
        pl.semaphore_wait(barrier, 4)

    def phase(thin, fat, wide, acc, out, cols, arr):
        tile = wide.shape[-1]
        tiles = ff // tile
        sent = tiles - 1 if cols else tiles

        def load(t, s):
            k = pl.multiple_of((t % blocks) * KBLOCK, KBLOCK)
            n = pl.multiple_of((t // blocks) * tile, tile)
            return (pltpu.make_async_copy(thin.at[pl.ds(k, KBLOCK)], narrow.at[s], s_n.at[s]),
                    pltpu.make_async_copy(fat.at[pl.ds(k, KBLOCK), pl.ds(n, tile)], wide.at[s], s_w.at[s]))

        def place(i):
            n = pl.multiple_of(i * tile, tile)
            return out.at[c, :, pl.ds(n, tile)] if cols else out.at[c, pl.ds(n, tile)]

        def keep_local(i, slot):
            return pltpu.make_async_copy(acc.at[slot], place(i), s_keep.at[arr, slot])

        def keep_remote(i, slot):
            return pltpu.make_async_remote_copy(acc.at[slot], place(i), s_keep.at[arr, slot], s_in.at[arr, c],
                                                device_id=here, device_id_type=MESH)

        def send(i, slot):
            return pltpu.make_async_remote_copy(acc.at[slot], place(i), s_send.at[arr, slot], s_in.at[arr, c],
                                                device_id=there, device_id_type=MESH)

        def detour(slot):
            return pltpu.make_async_remote_copy(acc.at[slot], via1, s_send.at[arr, slot], s_via.at[0],
                                                device_id=(dp, 2 + c), device_id_type=MESH)

        def rest_local(slot):
            return pltpu.make_async_copy(acc.at[slot], rest, s_keep.at[arr, slot])

        def drain(i, slot):
            send(i, slot).wait_send()

            @pl.when(jnp.logical_not(own))
            def _():
                keep_remote(i, slot).wait_send()

            @pl.when(own)
            def _():
                keep_local(i, slot).wait()

        for ahead in range(DEPTH - 1):
            for cp in load(ahead, ahead):
                cp.start()

        def step(t, carry):
            s = t % DEPTH
            i = t // blocks
            k = t % blocks
            slot = i % SLOTS

            @pl.when(k == 0)
            def _():
                @pl.when(i >= SLOTS)
                def _():
                    drain(i - SLOTS, slot)
                acc[slot] = jnp.zeros(acc.shape[1:], F32)
            for cp in load(t, s):
                cp.wait()

            @pl.when(t + DEPTH - 1 < tiles * blocks)
            def _():
                for cp in load(t + DEPTH - 1, (t + DEPTH - 1) % DEPTH):
                    cp.start()
            lhs, rhs = (narrow, wide) if cols else (wide, narrow)
            for q in range(acc.shape[1] // 256):
                rows = slice(q * 256, (q + 1) * 256)
                acc[slot, rows, :] += lax.dot_general(lhs[s, :, rows], rhs[s], (((0,), (0,)), ((), ())),
                                                      preferred_element_type=F32)

            if sent < tiles:
                @pl.when(t == tiles * blocks - 1)
                def _():
                    rest_local(slot).start()

            @pl.when((k == blocks - 1) & (i < sent))
            def _():
                if cols:
                    send(i, slot).start()
                else:
                    around = (xx == 0) & (i == DETOUR)

                    @pl.when(jnp.logical_not(around))
                    def _():
                        send(i, slot).start()

                    @pl.when(around)
                    def _():
                        detour(slot).start()

                @pl.when(own)
                def _():
                    keep_local(i, slot).start()

                @pl.when(jnp.logical_not(own))
                def _():
                    keep_remote(i, slot).start()
            return carry

        lax.fori_loop(0, tiles * blocks, step, 0)
        for i in range(tiles - SLOTS, sent):
            late.append(functools.partial(drain, i, i % SLOTS))
        if sent < tiles:
            late.append(lambda: rest_local((tiles - 1) % SLOTS).wait())

    late = []
    relay1 = pltpu.make_async_remote_copy(via1, via2, s_relay.at[0], s_via.at[1],
                                          device_id=(1 - dp, 2 + c), device_id_type=MESH)
    relay2 = pltpu.make_async_remote_copy(via2, dw2.at[c, pl.ds(DETOUR * TILE2, TILE2)], s_relay.at[1], s_in.at[1, c],
                                          device_id=(dp, 1 - dp), device_id_type=MESH)
    phase(g, a, wide2, acc2, dw2, False, 1)

    @pl.when(xx == 1)
    def _():
        pltpu.make_async_copy(via1, via1, s_via.at[0]).wait()
        relay1.start()
    phase(h, e, wide1, acc1, dw1, True, 0)

    @pl.when(xx == 1)
    def _():
        pltpu.make_async_copy(via2, via2, s_via.at[1]).wait()
        relay2.start()
    for wait in late:
        wait()

    @pl.when(xx == 1)
    def _():
        relay1.wait_send()
        relay2.wait_send()

    for j in (0, 1):
        @pl.when(jnp.logical_not(own) | (c != j))
        def _():
            part = dw1.at[j, :, pl.ds(0, ff - TILE1)]
            pltpu.make_async_copy(part, part, s_in.at[0, j]).wait()
            pltpu.make_async_copy(dw2.at[j], dw2.at[j], s_in.at[1, j]).wait()


def _gradients(h, e, a, g):
    tokens, d = h.shape
    ff = e.shape[1]
    any_ = pl.BlockSpec(memory_space=pl.ANY)
    dma = pltpu.SemaphoreType.DMA
    return pl.pallas_call(
        _grad_kernel,
        out_shape=(jax.ShapeDtypeStruct((2, d, ff), F32), jax.ShapeDtypeStruct((2, ff, d), F32),
                   jax.ShapeDtypeStruct((d, TILE1), F32),
                   jax.ShapeDtypeStruct((TILE2, d), F32), jax.ShapeDtypeStruct((TILE2, d), F32)),
        in_specs=[any_] * 4,
        out_specs=[any_] * 5,
        scratch_shapes=[
            pltpu.VMEM((DEPTH, KBLOCK, d), BF), pltpu.VMEM((DEPTH, KBLOCK, TILE1), BF),
            pltpu.VMEM((DEPTH, KBLOCK, TILE2), BF), pltpu.VMEM((SLOTS, d, TILE1), F32), pltpu.VMEM((SLOTS, TILE2, d), F32),
            dma((DEPTH,)), dma((DEPTH,)), dma((2, SLOTS)), dma((2, SLOTS)), dma((2, 2)), dma((2,)), dma((2,)),
        ],
        compiler_params=pltpu.CompilerParams(collective_id=1, has_side_effects=True, vmem_limit_bytes=67043328),
        cost_estimate=pl.CostEstimate(flops=4 * tokens * d * ff, bytes_accessed=4 * tokens * ff, transcendentals=0),
    )(h, e, a, g)


def _copy_kernel(a, b, a_out, b_out):
    a_out[...] = a[...]
    b_out[...] = b[...]


def _copies(dw1, dw2):
    _, d, ff = dw1.shape
    specs = [pl.BlockSpec((1, d // 8, ff - TILE1), lambda j, i: (j, i, 0)),
             pl.BlockSpec((1, ff // 8, d), lambda j, i: (j, i, 0))]
    return pl.pallas_call(
        _copy_kernel,
        grid=(2, 8),
        out_shape=(jax.ShapeDtypeStruct(dw1.shape, F32), jax.ShapeDtypeStruct(dw2.shape, F32)),
        in_specs=specs,
        out_specs=specs,
        cost_estimate=pl.CostEstimate(flops=10 ** 11, bytes_accessed=32 * d * ff, transcendentals=0),
    )(dw1, dw2)


def solution(mesh):
    def flat(x, y, c):
        return y * 4 + 2 * x + c

    chips = [(x, y) for x in (0, 1) for y in (0, 1)]
    keep = [[(flat(x, y, j), flat(x, y, 1 - j)) for x, y in chips if (x + y) % 2 != j] for j in (0, 1)]
    swap = [[(flat(x, y, j), flat(x, 1 - y, (x + y) % 2)) for x, y in chips] for j in (0, 1)]

    def body(x, t, w1, w2):
        nm, tok, d = x.shape
        ff = w1.shape[-1]
        inv = 1.0 / (nm * tok * mesh.shape['dp'] * d)
        xs = x.reshape(nm * tok // ROWS, ROWS, d)
        ts = t.reshape(nm * tok // ROWS, ROWS, d)
        hb, _, ab, eb, gb, _, _, _, ls = _forward_backward(xs, ts, w1[0], w2[0], inv)
        n = hb.shape[0] * ROWS
        dw1, dw2, rest, _, _ = _gradients(hb.reshape(n, d), eb.reshape(n, ff), ab.reshape(n, ff), gb.reshape(n, d))
        pp = lax.axis_index('pp')
        own = (pp // 2 + lax.axis_index('dp')) % 2 == pp % 2
        there = [lax.ppermute(rest, ('dp', 'pp'), swap[j]) for j in (0, 1)]
        here = [lax.ppermute(rest, ('dp', 'pp'), keep[j]) for j in (0, 1)]
        dw1, dw2 = _copies(dw1, dw2)
        for j in (0, 1):
            part = jnp.where(own, jnp.where(pp % 2 == j, rest, here[j]), there[j])
            dw1 = lax.dynamic_update_slice(dw1, part[None], (j, 0, ff - TILE1))
        loss = 0.5 * inv * jnp.sum(ls)
        return dw1[None], dw2[None], loss

    return jax.shard_map(body, mesh=mesh,
                         in_specs=(P(None, 'dp', None), P(None, 'dp', None), P('pp'), P('pp')),
                         out_specs=(P('pp'), P('pp'), P()), check_vma=False)
```
